256 devices in a mesh: groups: 4 (over y, x), expert: 64 (over z, core).
Axes of the slice: x: 2, y: 2, z: 32, core: 2. Of those that a mesh axis runs over, the one named last changes fastest.
The devices are a block of a 4x8x32 slice.
Arguments:
- tokens: bfloat16 [32768, 4096], P(('groups', 'expert')), parts along dimension 0, may hold values from -6 to 6
- router_weight: bfloat16 [4096, 128], replicated, may hold values from -0.078125 to 0.078125
- expert_ids: int32 [32768, 8], P(('groups', 'expert')), parts along dimension 0, may hold values from 0 to 127, all different within a row; in each aligned block of 128 rows (0 to 127, 128 to 255, ...) at most 9 rows name the same one
Outputs:
- expert_rows: bfloat16 [128, 2304, 4096], P('expert', 'groups'), parts along dimension 1
- balance_loss: float32 [4], P('groups'), parts along dimension 0
The draws below stay inside these ranges and needn't reach their ends.
There are 4 independent parts, one for each index of `groups`. The reference program is written for one: setup_inputs(seed, part) draws one part's arguments, and reference() takes and returns one part's arrays. A program takes and returns all parts, laid end to end along the dimension named above; an argument that names none is the same for every part. Nothing has to cross between parts.
Inputs may be any that keep to these rules, and one draw needn't show every extreme that they name: `expert_ids`: each row names 8 different experts; among the rows of one device no expert is named more than 9 times, a bound that some block reaches.
All inputs are finite; a program needn't handle non-finite values.
Results may differ from the reference program's by a relative error of at most 0.0012.
Values may be sent and summed in bfloat16 or wider, within the bound.
A program may use at most 128 MiB of HBM per device.

```python
import math
import jax
import jax.numpy as jnp
import numpy as np

D = 4096
EXPERTS = 128
TOP_K = 8
TOK_DEV = 128
CAP = 9
TOKENS = 8192
SLOTS = 576
N_EXPERT = 64


def pattern_signs(count):
    index = jnp.arange(count, dtype=jnp.int32)
    parity = jnp.zeros((count,), jnp.int32)
    for bit_place in range(20):
        parity = parity + jnp.bitwise_and(jnp.right_shift(index, bit_place), 1)
    return 1.0 - 2.0 * jnp.bitwise_and(parity, 1).astype(jnp.float32)


def draw_router_weight(key, part):
    first = jax.random.fold_in(key, 11)
    second = jax.random.fold_in(key, 12)
    noise = jnp.clip(jax.random.normal(first, (D, EXPERTS), jnp.float32), -4.0, 4.0)
    amplitude = jax.random.uniform(second, (EXPERTS,), jnp.float32, 0.3, 1.0)
    combined = (noise + amplitude[None, :] * pattern_signs(D)[:, None]) * D ** (-0.5)
    return combined.astype(jnp.bfloat16)


def draw_tokens(key, part):
    first = jax.random.fold_in(key, 21)
    second = jax.random.fold_in(key, 22)
    third = jax.random.fold_in(key, 23)
    rise = jnp.arange(TOKENS, dtype=jnp.float32) / max(TOKENS - 1, 1)
    base = jnp.clip(jax.random.normal(first, (TOKENS, D), jnp.float32), -6.0, 6.0)
    share = 1.0 / 32.0 * jnp.exp(rise * jnp.log(8.0))
    chosen_rows = jax.random.uniform(second, (TOKENS,), jnp.float32) < share
    strength = jax.random.randint(third, (TOKENS,), 2, 7).astype(jnp.float32)
    planted = strength[:, None] * pattern_signs(D)[None, :]
    return jnp.where(chosen_rows[:, None], planted, base).astype(jnp.bfloat16)


def deal_out(rng, own, number, rows, number_of, top, reach, lean):
    order = jax.random.permutation(rng, number_of)
    crowded, usual = load_shares(number_of, rows * top, reach, lean, True), load_shares(number_of, rows * top, reach, lean, False)
    places = jnp.arange(number_of)

    def named(tallies, offset_by):
        used = int((tallies > 0).sum())
        fixed = max(1, used // 4)
        moved = fixed + (places - fixed + offset_by * (used - fixed)) % max(1, number_of - fixed)
        return jnp.zeros((number_of,), jnp.int32).at[order[jnp.where(places < fixed, places, moved)]].set(jnp.asarray(tallies, jnp.int32))

    tallies = jnp.where(number % 4 == 0, named(crowded, number // 4), named(usual, number - number // 4 - 1))
    mixed = jax.random.permutation(jax.random.fold_in(own, 3), number_of)
    giver, receiver = mixed[0:number_of // 2 * 2:2], mixed[1:number_of // 2 * 2:2]
    slack = jnp.minimum(tallies[giver] - 1, reach - tallies[receiver]) // 2
    slack = jnp.where((giver == order[0]) | (receiver == order[0]) | (tallies[receiver] == 0), 0, jnp.maximum(slack, 0))
    moved = jax.random.randint(jax.random.fold_in(own, 4), (number_of // 2,), 0, 1 << 20) % (slack + 1)
    tallies = tallies.at[giver].add(-moved).at[receiver].add(moved)
    members = jnp.searchsorted(jnp.cumsum(tallies), jnp.arange(rows * top), side="right").astype(jnp.int32)
    listing = members.reshape(top, rows).T
    listing = listing[jax.random.permutation(jax.random.fold_in(own, 1), rows)]
    offset_by = jax.random.randint(jax.random.fold_in(own, 2), (rows, 1), 0, top)
    return jnp.take_along_axis(listing, (jnp.arange(top)[None, :] + offset_by) % top, axis=1)


def load_shares(count, total, bound, skew, full):
    weights = [(1 << 20) // math.isqrt(standing ** skew) + 1 for standing in range(1, count + 1)]
    largest = bound if full else min(bound, max(-(-total // count), total * weights[0] // sum(weights)))
    least = 1 if total - largest >= count - 1 else 0
    counts, surplus = [largest] + [least] * (count - 1), total - largest - least * (count - 1)
    while surplus > 0:
        candidates = [i for i in range(1, count) if counts[i] < largest] or [i for i in range(1, count) if counts[i] < bound]
        mass, left = sum([weights[i] for i in candidates]), surplus
        for i in candidates:
            more = min(bound - counts[i], max(1, left * weights[i] // mass), surplus)
            counts[i] = counts[i] + more
            surplus = surplus - more
    return np.array(counts)


def setup_inputs(seed: int = 0, part: int = 0) -> dict:
    keys = jax.random.split(jax.random.key(seed), 4)
    part_splits = jax.random.split(jax.random.fold_in(keys[3], part), 4)
    tokens = draw_tokens(jax.random.fold_in(jax.random.fold_in(keys[3], part), 71), part)
    router_weight = draw_router_weight(jax.random.fold_in(keys[3], 71), part)
    expert_ids_keys = jax.random.split(jax.random.fold_in(part_splits[2], 1), TOKENS // TOK_DEV)
    expert_ids_turns = jax.random.permutation(jax.random.fold_in(part_splits[2], 3), TOKENS // TOK_DEV)
    expert_ids = jax.vmap(lambda own, number: deal_out(jax.random.fold_in(part_splits[2], 2), own, number, TOK_DEV, EXPERTS, TOP_K, CAP, 2))(expert_ids_keys, expert_ids_turns).reshape((TOKENS, TOP_K))
    return dict(tokens=tokens, router_weight=router_weight, expert_ids=expert_ids)


def reference(tokens, router_weight, expert_ids):
    logits = jnp.dot(tokens, router_weight, preferred_element_type=jnp.float32)
    probability = jax.nn.softmax(logits, axis=-1)
    chosen = jnp.take_along_axis(logits, expert_ids, axis=1)
    gates = jax.nn.softmax(chosen, axis=1)
    onehot = jnp.sum((expert_ids[:, :, None] == jnp.arange(EXPERTS, dtype=jnp.int32)[None, None, :]).astype(jnp.int32), axis=1).astype(jnp.int32)
    blocks = onehot.reshape(N_EXPERT, TOK_DEV, EXPERTS)
    before = (jnp.cumsum(blocks, axis=1) - blocks).astype(jnp.int32).reshape(TOKENS, EXPERTS)
    slot_rank = jnp.take_along_axis(before, expert_ids, axis=1).astype(jnp.int32)
    owner_index = (jnp.arange(TOKENS, dtype=jnp.int32) // TOK_DEV)[:, None]
    position = (owner_index * CAP + slot_rank).astype(jnp.int32)
    widened = tokens.astype(jnp.float32)
    expert_rows = jnp.zeros((EXPERTS, SLOTS, D), jnp.bfloat16)
    for column in range(TOP_K):
        gated = (gates[:, column:column + 1] * widened).astype(jnp.bfloat16)
        expert_rows = expert_rows.at[expert_ids[:, column], position[:, column]].set(gated)
    expert_load = jnp.sum(onehot, axis=0).astype(jnp.float32)
    expert_mass = jnp.sum(probability, axis=0)
    token_total = jnp.float32(TOKENS)
    balance_loss = EXPERTS * jnp.sum(expert_load * expert_mass) / (token_total * token_total * TOP_K)
    return expert_rows, balance_loss.reshape(1)
```

```python
import jax
import jax.numpy as jnp
from jax import lax
from jax.experimental import pallas as pl
from jax.experimental.pallas import tpu as pltpu
from jax.sharding import PartitionSpec as P

CAP = 9
LOCAL = 2
CORES = 2
CHIP_SLOTS = CORES * LOCAL * CAP
WINDOW = 32
PIECES = 4
META = PIECES
TAIL = (0, 48, 80, 112)
COLS = 512
F32 = jnp.float32
MESH = pl.DeviceIdType.MESH


def kernel(
    ids_ref, tokens_hbm, weight_hbm,
    out_hbm, loss_ref,
    blocks, tail_long, tail_short, other, metas, other_meta, weight, rows_out, sums, other_sums,
    local_sem, piece_send, piece_recv, pass_send, pass_recv, free_sem, sum_sems,
):
    me = lax.axis_index("expert")
    chips = lax.axis_size("expert") // CORES
    tok = blocks.shape[1]
    width = blocks.shape[2]
    experts = weight.shape[1]
    part = tok // PIECES
    z = me // CORES
    core = me % CORES
    sign = 1 - 2 * core
    far_long = chips // 2
    far_short = chips - 1 - far_long
    sibling = CORES * z + 1 - core
    dirs = (sign, -sign)
    fars = (far_long, far_short)

    def chip_at(distance):
        return lax.rem(z + distance + 2 * chips, chips)

    def to(d):
        return {"expert": CORES * chip_at(dirs[d]) + core}

    def source(d, s):
        return chip_at(-dirs[d] * s)

    load_tokens = pltpu.make_async_copy(tokens_hbm, blocks.at[z], local_sem.at[0])
    load_weight = pltpu.make_async_copy(weight_hbm, weight, local_sem.at[1])
    load_tokens.start()
    load_weight.start()
    barrier = pltpu.get_barrier_semaphore()
    for peer in (to(0), to(1), {"expert": sibling}):
        pl.semaphore_signal(barrier, inc=1, device_id=peer, device_id_type=MESH)
    pl.semaphore_wait(barrier, 3)

    def piece(d, s, k, src, dst):
        return pltpu.make_async_remote_copy(
            src_ref=src, dst_ref=dst,
            send_sem=piece_send.at[d, lax.rem(s, 2), k],
            recv_sem=piece_recv.at[d, s - 1, k],
            device_id=to(d), device_id_type=MESH,
        )

    def full(d, s, k):
        c = source(d, s - 1)
        ref = metas.at[c] if k == META else blocks.at[c, pl.ds(k * part, part)]
        return piece(d, s, k, ref, ref)

    def tail(d, s, k, ref=None):
        c = source(d, s - 1)
        rows = pl.ds(TAIL[k], TAIL[k + 1] - TAIL[k])
        dst = blocks.at[c, rows]
        return piece(d, s, k, dst if ref is None else ref.at[rows], dst)

    def passed(d, c, rows):
        return (
            pltpu.make_async_remote_copy(
                src_ref=blocks.at[c, pl.ds(0, rows)], dst_ref=other.at[d, pl.ds(0, rows)],
                send_sem=pass_send.at[d, 0], recv_sem=pass_recv.at[d, 0],
                device_id={"expert": sibling}, device_id_type=MESH,
            ),
            pltpu.make_async_remote_copy(
                src_ref=metas.at[c], dst_ref=other_meta.at[d],
                send_sem=pass_send.at[d, 1], recv_sem=pass_recv.at[d, 1],
                device_id={"expert": sibling}, device_id_type=MESH,
            ),
        )

    def pass_on(d, c, rows, first):
        if not first:
            pl.semaphore_wait(free_sem.at[d], 1)
        for copy in passed(d, c, rows):
            copy.start()

    def take_pass(d, c, rows):
        for copy in passed(d, c, rows):
            copy.wait_recv()

    def end_pass(d, c, rows, last):
        for copy in passed(d, c, rows):
            copy.wait_send()
        if not last:
            pl.semaphore_signal(free_sem.at[d], inc=1, device_id={"expert": sibling},
                                device_id_type=MESH)

    def matches(target, meta):
        hit = jnp.zeros(target.shape, F32)
        gate = jnp.zeros(target.shape, F32)
        for k in range(8):
            same = target == meta[k : k + 1, :]
            hit = jnp.where(same, 1.0, hit)
            gate = jnp.where(same, meta[8 + k : 9 + k, :], gate)
        return hit.astype(jnp.bfloat16), jnp.sum(gate, axis=1, keepdims=True)

    def window_of(c, cc, lanes):
        start = CORES * CAP * c
        base = start // 16
        row = lax.broadcasted_iota(jnp.int32, (LOCAL * WINDOW, lanes), 0)
        expert = row // WINDOW
        rank = row % WINDOW - (start + CAP * cc - base * 16)
        return pl.multiple_of(base * 16, 16), expert, rank, (rank >= 0) & (rank < CAP)

    def place(first_row, pick, src, gate):
        def columns(n, carry):
            at = pl.ds(pl.multiple_of(n * COLS, COLS), COLS)
            got = jnp.dot(pick, src[:, at], preferred_element_type=F32)
            if gate is not None:
                got = got * gate
            got = got.astype(jnp.bfloat16)
            for e in range(LOCAL):
                there = (e, pl.ds(first_row, WINDOW), at)
                rows_out[there] = rows_out[there] + got[e * WINDOW : (e + 1) * WINDOW]
            return carry

        lax.fori_loop(0, width // COLS, columns, 0)

    def use_full(c, cc, src, meta_ref):
        first_row, expert, rank, ok = window_of(c, cc, tok)
        target = jnp.where(ok, (LOCAL * me + expert) * CAP + rank, -1).astype(F32)
        pick, gate = matches(target, meta_ref[...])
        place(first_row, pick, src, gate)

    def use_tail(c, cc, src, far, rows):
        first_row, expert, rank, ok = window_of(c, cc, rows)
        target = jnp.where(ok, CHIP_SLOTS * far + (LOCAL * core + expert) * CAP + rank, -1)
        lane = lax.broadcasted_iota(jnp.int32, target.shape, 1)
        pick = jnp.where(target == lane, 1.0, 0.0).astype(jnp.bfloat16)
        place(first_row, pick, src.at[pl.ds(0, rows)], None)

    def cut_down(d, c, ref):
        row = lax.broadcasted_iota(jnp.int32, (TAIL[-1], tok), 0)
        target = jnp.full(row.shape, -1, jnp.int32)
        for q in range(3):
            chip = chip_at(dirs[d] * (3 - q))
            inside = (row >= q * CHIP_SLOTS) & (row < (q + 1) * CHIP_SLOTS)
            target = jnp.where(inside, chip * CHIP_SLOTS + row - q * CHIP_SLOTS, target)
        pick, gate = matches(target.astype(F32), metas[c])

        def columns(n, carry):
            at = pl.ds(pl.multiple_of(n * COLS, COLS), COLS)
            got = jnp.dot(pick, blocks[c, :, at], preferred_element_type=F32) * gate
            ref[:, at] = got.astype(jnp.bfloat16)
            return carry

        lax.fori_loop(0, width // COLS, columns, 0)

    load_tokens.wait()
    for k in range(PIECES):
        for d in range(2):
            full(d, 1, k).start()

    load_weight.wait()
    logits = jnp.zeros((tok, experts), F32)
    for n in range(0, width, COLS):
        logits += jnp.dot(blocks[z, :, n : n + COLS], weight[n : n + COLS, :],
                          preferred_element_type=F32)
    raised = jnp.exp(logits - jnp.max(logits, axis=1, keepdims=True))
    probability = raised / jnp.sum(raised, axis=1, keepdims=True)
    mass = jnp.sum(probability, axis=0, keepdims=True)
    by_expert = logits.T
    ids = ids_ref[...]
    expert_row = lax.broadcasted_iota(jnp.int32, (experts, tok), 0)
    token_lane = lax.broadcasted_iota(jnp.int32, (experts, tok), 1)
    named = jnp.zeros((experts, tok), F32)
    for k in range(8):
        named = jnp.where(expert_row == ids[k : k + 1, :], 1.0, named)
    named16 = named.astype(jnp.bfloat16)
    earlier = (lax.broadcasted_iota(jnp.int32, (tok, tok), 0)
               < lax.broadcasted_iota(jnp.int32, (tok, tok), 1))
    before = jnp.dot(named16, jnp.where(earlier, 1.0, 0.0).astype(jnp.bfloat16),
                     preferred_element_type=F32)
    load = lax.dot_general(jnp.ones((8, tok), jnp.bfloat16), named16,
                           (((1,), (1,)), ((), ())), preferred_element_type=F32)[0:1]
    slots = []
    chosen = []
    for k in range(8):
        same = expert_row == ids[k : k + 1, :]
        rank = jnp.sum(jnp.where(same, before, 0.0), axis=0, keepdims=True)
        slots.append(ids[k : k + 1, :].astype(F32) * CAP + rank)
        chosen.append(jnp.sum(jnp.where(same, by_expert, 0.0), axis=0, keepdims=True))
    chosen = jnp.concatenate(chosen, axis=0)
    lifted = jnp.exp(chosen - jnp.max(chosen, axis=0, keepdims=True))
    gates = lifted / jnp.sum(lifted, axis=0, keepdims=True)
    metas[z, 0:8, :] = jnp.concatenate(slots, axis=0)
    metas[z, 8:16, :] = gates
    which = lax.broadcasted_iota(jnp.int32, (8, experts), 0)
    metas[z, 16:24, :] = jnp.where(which == 0, load, jnp.where(which == 1, mass, 0.0))

    for n in range(0, rows_out.shape[1], WINDOW):
        for e in range(LOCAL):
            rows_out[e, n : n + WINDOW, :] = jnp.zeros((WINDOW, width), jnp.bfloat16)

    for d in range(2):
        full(d, 1, META).start()
    pass_on(0, z, tok, True)
    use_full(z, core, blocks.at[z], metas.at[z])
    take_pass(0, z, tok)
    use_full(z, 1 - core, other.at[0], other_meta.at[0])
    end_pass(0, z, tok, False)

    def is_full(d, s):
        return s <= fars[d] - 3

    def tail_parts(d, s):
        return fars[d] - s + 1

    def arrive(d, s, k):
        (full if is_full(d, s) else tail)(d, s, k).wait_recv()

    def settle(d, s, k, static):
        if static and (s < 1 or s > fars[d]):
            return
        if static and not is_full(d, s) and k != META and k >= tail_parts(d, s):
            return
        (full if not static or is_full(d, s) or k == META else tail)(d, s, k).wait_send()

    TAIL_AT = {TAIL[n]: n - 1 for n in (1, 2, 3)}

    def handle(ways, s):
        for d, rows, first, last in ways:
            c = source(d, s)
            if rows == tok:
                use_full(c, core, blocks.at[c], metas.at[c])
            else:
                use_tail(c, core, blocks.at[c], TAIL_AT[rows], rows)
        for d, rows, first, last in ways:
            c = chip_at(dirs[d] * s)
            take_pass(d, c, rows)
            if rows == tok:
                use_full(c, 1 - core, other.at[d], other_meta.at[d])
            else:
                use_tail(c, 1 - core, other.at[d], TAIL_AT[rows], rows)
            end_pass(d, c, rows, last)

    def both_full(s, carry):
        for k in range(PIECES + 1):
            for d in range(2):
                full(d, s, k).wait_recv()
                full(d, s, k).wait_send()
                full(d, s + 1, k).start()
        for d in range(2):
            pass_on(d, source(d, s), tok, False)
        handle([(d, tok, False, False) for d in range(2)], s)
        return carry

    pl.semaphore_signal(free_sem.at[1], inc=1, device_id={"expert": sibling}, device_id_type=MESH)
    lax.fori_loop(1, far_short - 3, both_full, 0)

    for s in range(far_short - 3, far_long + 1):
        ways = []
        for d in range(2):
            if s > fars[d]:
                continue
            rows = tok if is_full(d, s) else TAIL[tail_parts(d, s)]
            ways.append((d, rows, False, s == fars[d]))
        for k in range(PIECES + 1):
            for d, rows, first, last in ways:
                if k == META or is_full(d, s) or k < tail_parts(d, s):
                    (full if k == META or is_full(d, s) else tail)(d, s, k).wait_recv()
                    settle(d, s, k, True)
                    if s < fars[d] and (k == META or is_full(d, s + 1)):
                        full(d, s + 1, k).start()
                    elif s < fars[d] and not is_full(d, s) and k < tail_parts(d, s + 1):
                        tail(d, s + 1, k).start()
        for d, rows, first, last in ways:
            if s == fars[d] - 3:
                ref = tail_short if d else tail_long
                cut_down(d, source(d, s), ref)
                for k in range(3):
                    tail(d, s + 1, k, ref).start()
        for d, rows, first, last in ways:
            pass_on(d, source(d, s), rows, False)
        handle(ways, s)

    total = metas[0, 16:24, :]
    for c in range(1, chips):
        total = total + metas[c, 16:24, :]
    sums[...] = total
    swap = pltpu.make_async_remote_copy(
        src_ref=sums, dst_ref=other_sums, send_sem=sum_sems.at[0], recv_sem=sum_sems.at[1],
        device_id={"expert": sibling}, device_id_type=MESH,
    )
    swap.start()
    write = pltpu.make_async_copy(rows_out, out_hbm, local_sem.at[0])
    write.start()
    swap.wait()
    both = sums[...] + other_sums[...]
    tokens_all = F32(tok * chips * CORES)
    summed = jnp.sum(both[0:1] * both[1:2])
    loss_ref[0] = experts * summed / (tokens_all * tokens_all * 8)
    write.wait()


def on_device(tokens, router_weight, expert_ids):
    tok, width = tokens.shape
    experts = router_weight.shape[1]
    devices = lax.axis_size("expert")
    chips = devices // CORES
    bf16 = jnp.bfloat16
    dma = pltpu.SemaphoreType.DMA
    return pl.pallas_call(
        kernel,
        name="dispatch",
        out_shape=(
            jax.ShapeDtypeStruct((LOCAL, devices * CAP, width), bf16),
            jax.ShapeDtypeStruct((1,), F32),
        ),
        in_specs=[
            pl.BlockSpec(memory_space=pltpu.VMEM),
            pl.BlockSpec(memory_space=pl.ANY),
            pl.BlockSpec(memory_space=pl.ANY),
        ],
        out_specs=(
            pl.BlockSpec(memory_space=pl.ANY),
            pl.BlockSpec(memory_space=pltpu.SMEM),
        ),
        scratch_shapes=[
            pltpu.VMEM((chips, tok, width), bf16),
            pltpu.VMEM((TAIL[-1], width), bf16),
            pltpu.VMEM((TAIL[-1], width), bf16),
            pltpu.VMEM((2, tok, width), bf16),
            pltpu.VMEM((chips, 24, tok), F32),
            pltpu.VMEM((2, 24, tok), F32),
            pltpu.VMEM((width, experts), bf16),
            pltpu.VMEM((LOCAL, devices * CAP, width), bf16),
            pltpu.VMEM((8, experts), F32),
            pltpu.VMEM((8, experts), F32),
            dma((2,)),
            dma((2, 2, PIECES + 1)),
            dma((2, chips // 2, PIECES + 1)),
            dma((2, 2)),
            dma((2, 2)),
            pltpu.SemaphoreType.REGULAR((2,)),
            dma((2,)),
        ],
        compiler_params=pltpu.CompilerParams(
            collective_id=0, has_side_effects=True, vmem_limit_bytes=60 * 1024 * 1024
        ),
    )(expert_ids.T, tokens, router_weight)


def solution(mesh):
    both = ("groups", "expert")
    return jax.shard_map(
        on_device, mesh=mesh, in_specs=(P(both, None), P(), P(both, None)),
        out_specs=(P("expert", "groups", None), P("groups")), check_vma=False,
    )
```
